32 devices in a mesh: grp: 4 (over y, x), seq: 8 (over z, core).
Axes of the slice: x: 2, y: 2, z: 4, core: 2. Of those that a mesh axis runs over, the one named last changes fastest.
Arguments:
- tokens: bfloat16 [2048, 8192], P(None, 'seq'), may hold values from -16 to 16
- proj_weight: bfloat16 [8192, 5120], P('seq', 'grp'), may hold values from -0.0625 to 0.0625
- proj_bias: bfloat16 [5120], P('grp'), may hold values from -3 to 3
- out_weight: bfloat16 [4096, 8192], P('grp'), may hold values from -0.125 to 0.125
- doc_ids: int32 [2048], P('seq'), may hold values from 0 to 2, never falling along the last dimension, each value on 1 to 1280 neighbouring positions
Outputs:
- mixed: bfloat16 [2048, 8192], P('seq', 'grp')
The draws below stay inside these ranges and needn't reach their ends.
Inputs may be any that keep to these rules, and one draw needn't show every extreme that they name: `doc_ids`: numbers never fall along the sequence; every document has 1 to 1280 tokens, one exactly that many; every number up to 2 is used.
All inputs are finite; a program needn't handle non-finite values.
Results may differ from the reference program's by a relative error of at most 0.012.
Values may be sent and summed in bfloat16 or wider, within the bound.
A program may use at most 256 MiB of HBM per device.

```python
import math
import jax
import jax.numpy as jnp
import numpy as np
from jax import lax

D = 8192
Q_HEADS = 32
KV_HEADS = 4
HEAD_DIM = 128
TOK_DEV = 256
SPAN = 5
GQA = 8
TOKENS = 2048
DOCS = 3


def draw_tokens(key, part):
    normals = jax.random.normal(jax.random.fold_in(key, 11), (TOKENS, D), jnp.float32)
    block_offsets = jax.random.normal(jax.random.fold_in(key, 19), (TOKENS // TOK_DEV, D), jnp.float32)
    offset_rows = jnp.repeat(block_offsets, TOK_DEV, axis=0)
    result = jnp.clip(normals + 1.5 * offset_rows, -8.0, 8.0)
    return result.astype(jnp.bfloat16)


def with_spikes(drawn, own_key, source, target, shards_of, factor):
    owner, partner = [(jnp.arange(drawn.shape[position]) // (drawn.shape[position] // shards_of)).reshape([-1 if axis == position else 1 for axis in range(drawn.ndim)]) for position in (source, target)]
    chosen = jax.random.permutation(own_key, shards_of)[partner]
    strong = (owner == chosen) | (owner == (partner + shards_of // 2) % shards_of)
    return jnp.where(strong, factor * drawn, drawn)


def block_scale(own_key, extent, shards, low, largest):
    def one(axis_at, parts):
        draws = jax.random.uniform(jax.random.fold_in(jax.random.fold_in(own_key, 6), axis_at), (parts,), jnp.float32, low / len(shards), largest / len(shards))
        return jnp.repeat(jnp.exp(draws), extent[axis_at] // parts).reshape((-1,) + (1,) * (len(extent) - axis_at - 1))

    level = one(*shards[0])
    for cut in shards[1:]:
        level = level * one(*cut)
    return level


def split_up(number_of, total, limit, slope):
    weights = [(1 << 20) // math.isqrt(standing ** slope) + 1 for standing in range(2, number_of + 1)]
    spare, holding = total - limit - (number_of - 1), [1] * (number_of - 1)
    while spare > 0:
        movable = [i for i in range(number_of - 1) if holding[i] < limit]
        pool, remaining = sum([weights[i] for i in movable]), spare
        for i in movable:
            more = min(limit - holding[i], max(1, remaining * weights[i] // pool), spare)
            holding[i] = holding[i] + more
            spare = spare - more
    return np.array([limit] + holding)


def ragged_sizes(key, amount, total, limit, slope):
    if amount == 2:
        one = jax.random.randint(key, (), max(1, total - limit), min(limit, total - 1) + 1)
        return jnp.stack([one, total - one])
    sizes = jnp.asarray(split_up(amount, total, limit, slope), jnp.int32)
    twos = (amount - 1) // 2
    donor, sink = sizes[1:1 + 2 * twos:2], sizes[2:2 + 2 * twos:2]
    room = jnp.minimum(donor - 1, limit - sink)
    shifted = jax.random.randint(jax.random.fold_in(key, 1), (twos,), 0, 1 << 20) % (room + 1)
    sizes = sizes.at[1:1 + 2 * twos:2].set(donor - shifted).at[2:2 + 2 * twos:2].set(sink + shifted)
    return sizes[jax.random.permutation(jax.random.fold_in(key, 2), amount)]


def normal_values(rng, shape, scale, reach, split=(), held_as=jnp.bfloat16):
    drawn = jax.random.normal(rng, shape, jnp.float32) * scale
    if len(split) > 0:
        drawn = block_scale(rng, shape, split, -0.22, 0.18) * drawn
    return jnp.clip(drawn, min=-reach, max=reach).astype(held_as)


def bell_draw_with(own_key, extent, deviation, limit, split, heavy, kind=jnp.bfloat16):
    array = deviation * jax.random.normal(own_key, extent, jnp.float32)
    if split:
        array = array * block_scale(own_key, extent, split, -0.22, 0.18)
    return jnp.clip(with_spikes(array, jax.random.fold_in(own_key, 3), *heavy), -limit, limit).astype(kind)


def setup_inputs(seed: int = 0) -> dict:
    splits = jax.random.split(jax.random.key(seed), 6)
    tokens = draw_tokens(jax.random.fold_in(splits[5], 71), 0)
    proj_weight = normal_values(splits[1], (D, KV_HEADS * (GQA + 2) * HEAD_DIM), D ** -0.5, 0.0625, ((0, 8), (1, 4)))
    proj_bias = normal_values(splits[2], (KV_HEADS * (GQA + 2) * HEAD_DIM,), 0.5, 3.0, ((0, 4),))
    out_weight = bell_draw_with(splits[3], (Q_HEADS * HEAD_DIM, D), (Q_HEADS * HEAD_DIM) ** -0.5, 0.125, ((0, 4),), (0, 1, 4, 2.0))
    doc_ids = jnp.searchsorted(jnp.cumsum(ragged_sizes(splits[4], DOCS, TOKENS, SPAN * TOK_DEV, 1)), jnp.arange(TOKENS), side="right").astype(jnp.int32)
    return dict(tokens=tokens, proj_weight=proj_weight, proj_bias=proj_bias, out_weight=out_weight, doc_ids=doc_ids)


theta_base = 1000000.0


def rotate(inputs, positions, head_dim):
    half_dim = head_dim // 2
    inverse_freq = theta_base ** (-(jnp.arange(half_dim, dtype=jnp.float32) * 2.0) / head_dim)
    angles = positions.astype(jnp.float32)[:, None] * inverse_freq[None, :]
    cosine = jnp.concatenate([jnp.cos(angles), jnp.cos(angles)], axis=1)
    sine_table = jnp.concatenate([jnp.sin(angles), jnp.sin(angles)], axis=1)
    low_half = inputs[..., :half_dim]
    high_half = inputs[..., half_dim:]
    turned = jnp.concatenate([-high_half, low_half], axis=-1)
    return inputs * cosine[:, None, :] + turned * sine_table[:, None, :]


def reference(tokens, proj_weight, proj_bias, out_weight, doc_ids):
    projected = jnp.dot(tokens, proj_weight, preferred_element_type=jnp.float32) + proj_bias.astype(jnp.float32)[None, :]
    projected = projected.reshape(TOKENS, KV_HEADS, GQA + 2, HEAD_DIM)
    positions = jnp.arange(TOKENS, dtype=jnp.int32)
    queries = rotate(projected[:, :, :GQA, :].reshape(TOKENS, Q_HEADS, HEAD_DIM), positions, HEAD_DIM).astype(jnp.bfloat16)
    key_rows = rotate(projected[:, :, GQA, :], positions, HEAD_DIM).astype(jnp.bfloat16)
    value_rows = projected[:, :, GQA + 1, :].astype(jnp.bfloat16)
    allowed = (doc_ids[None, :] == doc_ids[:, None]) & (positions[None, :] <= positions[:, None])
    score_scale = HEAD_DIM ** -0.5

    def one_head(head_index):
        query_head = lax.dynamic_index_in_dim(queries, head_index, 1, keepdims=False).astype(jnp.float32)
        key_head = lax.dynamic_index_in_dim(key_rows, head_index // GQA, 1, keepdims=False).astype(jnp.float32)
        value_head = lax.dynamic_index_in_dim(value_rows, head_index // GQA, 1, keepdims=False)
        scores = jnp.dot(query_head, key_head.T, preferred_element_type=jnp.float32) * score_scale
        scores = jnp.where(allowed, scores, -jnp.inf)
        row_max = jnp.max(scores, axis=1, keepdims=True)
        weights = jnp.exp(scores - row_max)
        row_sum = jnp.sum(weights, axis=1, keepdims=True)
        summed = jnp.dot(weights.astype(jnp.bfloat16), value_head, preferred_element_type=jnp.float32)
        return (summed / row_sum).astype(jnp.bfloat16)

    head_outputs = lax.map(one_head, jnp.arange(Q_HEADS, dtype=jnp.int32))
    attended = jnp.transpose(head_outputs, (1, 0, 2)).reshape(TOKENS, Q_HEADS * HEAD_DIM)
    return jnp.dot(attended, out_weight, preferred_element_type=jnp.float32).astype(jnp.bfloat16)
```

```python
import functools

import jax
import jax.numpy as jnp
from jax import lax
from jax.experimental import pallas as pl
from jax.experimental.pallas import tpu as pltpu
from jax.sharding import PartitionSpec as P

HEAD_DIM = 128
GQA = 8
PIECES = 4
MESH = pl.DeviceIdType.MESH

theta_base = 1000000.0
neg_large = -1e30
log2_e = 1.4426950408889634


def layer_kernel(
    line, rows, width, groups, tiles, wide, slots,
    tok_ref, w_ref, bias_ref, freq_ref, ids_ref, ow_ref,
    out_ref,
    kpair_out, kpair_in, kline_in, qpair_out, qpair_in, qline_in, ktotal, qtotal,
    queries, kv_ref, attended, ids_col, idall_ref, bias, cos_ref, sin_ref,
    weights, kept, send1, recv1, send2, recv2,
    kpair_ss, kpair_rs, kline_ss, kline_rs, qpair_ss, qpair_rs, qline_ss, qline_rs,
    idl_ss, idl_rs, idp_ss, idp_rs, kvu_ss, kvd_ss, kvl_rs, kvp_ss, kvp_rs,
    w_sem, ss1, rs1, ss2, rs2,
):
    g = lax.axis_index("grp")
    s = lax.axis_index("seq")
    z, c = s // 2, lax.rem(s, 2)
    n = 2 * line
    partner = s + 1 - 2 * c
    above = lax.rem(s + 2, n)
    below = lax.rem(s + n - 2, n)
    low = z < line // 2
    inner = (z > 0) & (z < line - 1)
    hub = line // 2 - 1
    pieces = PIECES
    part = rows // pieces
    q_width = GQA * HEAD_DIM
    peer_x = g + 1 - 2 * lax.rem(g, 2)
    peer_y = lax.rem(g + 2, groups)
    passes = 4 * tiles
    resident = slots == passes
    bf16, f32 = jnp.bfloat16, jnp.float32

    def first_peer(t):
        return jnp.where(lax.rem(t, 2) == 0, peer_x, peer_y)

    def second_peer(t):
        return jnp.where(lax.rem(t, 2) == 0, peer_y, peer_x)

    def w_copy(m):
        pos, t = lax.rem(m // tiles, 4), lax.rem(m, tiles)
        block = jnp.where(
            pos == 0, groups - 1 - g, jnp.where(pos == 1, first_peer(t), jnp.where(pos == 2, g, second_peer(t)))
        )
        column = pl.multiple_of((block * tiles + t) * wide, wide)
        slot = lax.rem(m, slots)
        return pltpu.make_async_copy(ow_ref.at[:, pl.ds(column, wide)], weights.at[slot], w_sem.at[slot])

    @pl.loop(0, slots)
    def _(m):
        w_copy(m).start()

    barrier = pltpu.get_barrier_semaphore()
    for peer in ((g, partner), (peer_x, s), (peer_y, s)):
        pl.semaphore_signal(barrier, inc=1, device_id=peer, device_id_type=MESH)

    @pl.when(z < line - 1)
    def _():
        pl.semaphore_signal(barrier, inc=1, device_id=(g, above), device_id_type=MESH)

    @pl.when(z > 0)
    def _():
        pl.semaphore_signal(barrier, inc=1, device_id=(g, below), device_id_type=MESH)

    row_ids = jnp.broadcast_to(ids_ref[...].reshape(1, rows), (HEAD_DIM, rows))
    idall_ref[s] = row_ids[:8]
    ids_col[...] = row_ids.T
    bias[...] = jnp.broadcast_to(bias_ref[...].astype(f32), bias.shape)
    pl.semaphore_wait(barrier, 3 + (z > 0).astype(jnp.int32) + (z < line - 1).astype(jnp.int32))

    def remote(src, dst, ss, rs, peer):
        return pltpu.make_async_remote_copy(src, dst, ss, rs, device_id=peer, device_id_type=MESH)


    def kpair_copy(dest):
        return remote(kpair_out.at[dest], kpair_in.at[dest], kpair_ss.at[dest], kpair_rs.at[dest], (g, partner))

    def qpair_copy(p, dest):
        slot = lax.rem(p, 2)
        return remote(
            qpair_out.at[slot, dest], qpair_in.at[p, dest], qpair_ss.at[p, dest], qpair_rs.at[p, dest], (g, partner)
        )

    def kline_copy(up, dest):
        return remote(
            kpair_in.at[dest], kline_in.at[up, dest], kline_ss.at[dest], kline_rs.at[up, dest],
            (g, jnp.where(up == 1, above, below)),
        )

    def qline_copy(up, p, dest):
        return remote(
            qpair_in.at[p, dest], qline_in.at[p, dest + up], qline_ss.at[p, dest], qline_rs.at[p, dest + up],
            (g, jnp.where(up == 1, above, below)),
        )

    def kproduct(dest, core):
        row = pl.multiple_of((2 * dest + core) * rows, rows)
        return jnp.dot(tok_ref[pl.ds(row, rows), :], w_ref[:, q_width:], preferred_element_type=f32)

    def q_tokens(p, dest, core):
        return tok_ref[pl.ds(pl.multiple_of((2 * dest + core) * rows + p * part, part), part), :]

    def kpair_stage():
        @pl.loop(0, line)
        def _(i):
            dest = jnp.where(low, line - 1 - i, i)
            kpair_out[dest] = kproduct(dest, 1 - c).astype(bf16)
            kpair_copy(dest).start()

    def qpair_stage(p):
        @pl.loop(0, line // 4)
        def _(b):
            stacked = jnp.concatenate([q_tokens(p, 4 * b + i, 1 - c) for i in range(4)], axis=0)
            value = jnp.dot(stacked, w_ref[:, :q_width], preferred_element_type=f32).astype(bf16)

            @pl.when(p >= 2)
            def _():
                for i in range(4):
                    qpair_copy(p - 2, 4 * b + i).wait_send()

            for i in range(4):
                qpair_out[lax.rem(p, 2), 4 * b + i] = value[i * part : (i + 1) * part]
                qpair_copy(p, 4 * b + i).start()

    def kline_stage(up, enabled):
        count = jnp.where(up == 1, jnp.where(z < hub, line, line - 1 - z), jnp.where(z > hub, z, 0))

        @pl.loop(0, jnp.where(enabled, count, 0))
        def _(i):
            dest = jnp.where(up == 1, line - 1 - i, i)
            ktotal[...] = kproduct(dest, c)
            kpair_copy(dest).wait_recv()
            source = jnp.where(up == 1, z > 0, z < line - 1)

            @pl.when(source)
            def _():
                kline_copy(up, dest).wait_recv()
                kpair_in[dest] = (ktotal[...] + kpair_in[dest].astype(f32) + kline_in[up, dest].astype(f32)).astype(bf16)

            @pl.when(jnp.logical_not(source))
            def _():
                kpair_in[dest] = (ktotal[...] + kpair_in[dest].astype(f32)).astype(bf16)

            kline_copy(up, dest).start()

    def qline_stage(up, p, enabled):
        @pl.loop(0, jnp.where(enabled, jnp.where(up == 1, line - 1 - z, z), 0))
        def _(i):
            dest = jnp.where(up == 1, line - 1 - i, i)
            qtotal[...] = jnp.dot(q_tokens(p, dest, c), w_ref[:, :q_width], preferred_element_type=f32)
            qpair_copy(p, dest).wait_recv()
            source = jnp.where(up == 1, z > 0, z < line - 1)

            @pl.when(source)
            def _():
                qline_copy(up, p, dest).wait_recv()
                qpair_in[p, dest] = (
                    qtotal[...] + qpair_in[p, dest].astype(f32) + qline_in[p, dest + up].astype(f32)
                ).astype(bf16)

            @pl.when(jnp.logical_not(source))
            def _():
                qpair_in[p, dest] = (qtotal[...] + qpair_in[p, dest].astype(f32)).astype(bf16)

            qline_copy(up, p, dest).start()

    main = low.astype(jnp.int32)
    other = 1 - main
    end = jnp.logical_not(inner)


    def tables(slot, block):
        angles = (block * rows + lax.broadcasted_iota(jnp.int32, (rows, HEAD_DIM), 0)).astype(f32) * freq_ref[...]
        lane = lax.broadcasted_iota(jnp.int32, (rows, HEAD_DIM), 1)
        sine = jnp.sin(angles)
        cos_ref[slot] = jnp.cos(angles)
        sin_ref[slot] = jnp.where(lane < HEAD_DIM // 2, -sine, sine)

    def rope(x, cosine, sine):
        return x * cosine + pltpu.roll(x, HEAD_DIM // 2, 1) * sine


    def kv_up(zz):
        block = kv_ref.at[2 * zz + c]
        return remote(block, block, kvu_ss.at[zz], kvl_rs.at[zz], (g, above))

    def kv_down(zz):
        block = kv_ref.at[2 * zz + c]
        return remote(block, block, kvd_ss.at[zz], kvl_rs.at[zz], (g, below))

    def kv_pair(zz, core):
        block = kv_ref.at[2 * zz + core]
        return remote(block, block, kvp_ss.at[zz], kvp_rs.at[zz], (g, partner))

    def kv_finish(zz, slot):
        ktotal[...] = kproduct(zz, c)
        kpair_copy(zz).wait_recv()
        ktotal[...] += kpair_in[zz].astype(f32)

        @pl.when(z < line - 1)
        def _():
            kline_copy(0, zz).wait_recv()
            ktotal[...] += kline_in[0, zz].astype(f32)

        kline_copy(1, zz).wait_recv()
        value = ktotal[...] + kline_in[1, zz].astype(f32) + bias[:1, q_width:]
        kv_ref[2 * zz + c, :, :HEAD_DIM] = rope(value[:, :HEAD_DIM], cos_ref[slot], sin_ref[slot]).astype(bf16)
        kv_ref[2 * zz + c, :, HEAD_DIM:] = value[:, HEAD_DIM:].astype(bf16)

        @pl.when(z < line - 1)
        def _():
            kv_up(zz).start()

        @pl.when(zz < z)
        def _():
            kv_down(zz).start()

        kv_pair(zz, c).start()

    def kv_relay():
        @pl.loop(0, jnp.where(z > hub, z, 0))
        def _(i):
            zz = z - 1 - i
            kv_up(zz).wait_recv()

            @pl.when(z < line - 1)
            def _():
                kv_up(zz).start()

            kv_pair(zz, c).start()

        @pl.loop(0, jnp.where(z < hub, z + 1, 0))
        def _(i):
            zz = z - i
            kv_down(zz).wait_recv()

            @pl.when(zz < z)
            def _():
                kv_down(zz).start()

            kv_pair(zz, c).start()


    def id_up(zz):
        block = idall_ref.at[2 * zz + c]
        return remote(block, block, idl_ss.at[zz], idl_rs.at[zz], (g, above))

    def id_pair(zz, core):
        block = idall_ref.at[2 * zz + core]
        return remote(block, block, idp_ss.at[zz], idp_rs.at[zz], (g, partner))

    def id_send(zz):
        @pl.when(z < line - 1)
        def _():
            id_up(zz).start()

        id_pair(zz, c).start()

    def id_relay():
        @pl.loop(0, z)
        def _(i):
            zz = z - 1 - i
            id_up(zz).wait_recv()
            id_send(zz)


    def finish(p):
        qtotal[...] = jnp.dot(q_tokens(p, z, c), w_ref[:, :q_width], preferred_element_type=f32)
        qpair_copy(p, z).wait_recv()
        qtotal[...] += qpair_in[p, z].astype(f32)

        @pl.when(z < line - 1)
        def _():
            qline_copy(0, p, z).wait_recv()
            qtotal[...] += qline_in[p, z].astype(f32)

        @pl.when(z > 0)
        def _():
            qline_copy(1, p, z).wait_recv()
            qtotal[...] += qline_in[p, z + 1].astype(f32)

        mine = pl.ds(pl.multiple_of(p * part, part), part)
        cosine, sine = cos_ref[0, mine, :], sin_ref[0, mine, :]
        for head in range(GQA):
            lanes = slice(head * HEAD_DIM, (head + 1) * HEAD_DIM)
            value = rope(qtotal[:, lanes] + bias[:1, lanes], cosine, sine)
            queries[head * part : (head + 1) * part, :] = value.astype(bf16)

    def attend(p):
        heads = GQA // 2
        ahead = lax.broadcasted_iota(jnp.int32, (part, rows), 1) - lax.broadcasted_iota(jnp.int32, (part, rows), 0)
        ahead = ahead - p * part
        mine_ids = ids_col[pl.ds(pl.multiple_of(p * part, part), part), :1]
        ones = jnp.ones((rows, HEAD_DIM), bf16)
        scale = HEAD_DIM ** (-0.5) * log2_e
        stacked = [queries[i * heads * part : (i + 1) * heads * part, :] for i in range(2)]

        def step(j, state):
            keys = kv_ref[j, :, :HEAD_DIM]
            values = jnp.concatenate([kv_ref[j, :, HEAD_DIM:], ones], axis=1)
            allowed = (mine_ids == idall_ref[j, :1, :]) & (ahead <= (s - j) * rows)
            allowed = jnp.concatenate([allowed] * heads, axis=0)
            new = []
            for i in range(2):
                row_max, weighted = state[i]
                scores = lax.dot_general(
                    stacked[i], keys, (((1,), (1,)), ((), ())), preferred_element_type=f32
                )
                scores = jnp.where(allowed, scores * scale, neg_large)
                new_max = jnp.maximum(row_max, jnp.max(scores, axis=1, keepdims=True))
                exps = jnp.exp2(scores - new_max)
                update = jnp.dot(exps.astype(bf16), values, preferred_element_type=f32)
                new.append((new_max, weighted * jnp.exp2(row_max - new_max) + update))
            return tuple(new)

        initial = (
            jnp.full((heads * part, 1), neg_large, f32),
            jnp.zeros((heads * part, 2 * HEAD_DIM), f32),
        )
        state = lax.fori_loop(jnp.maximum(s - (line + 1), 0), s + 1, step, (initial, initial))
        for i in range(2):
            weighted = state[i][1]
            value = (weighted[:, :HEAD_DIM] / weighted[:, HEAD_DIM:]).astype(bf16)
            for h in range(heads):
                head = i * heads + h
                attended[:, head * HEAD_DIM : (head + 1) * HEAD_DIM] = value[h * part : (h + 1) * part]


    def mixed(p, pos, t):
        m = p * passes + pos * tiles + t
        slot = lax.rem(m, slots)
        if resident:
            @pl.when(p == 0)
            def _():
                w_copy(m).wait()
        else:
            w_copy(m).wait()
        value = jnp.dot(attended[...], weights[slot], preferred_element_type=f32)
        if not resident:
            @pl.when(m + slots < pieces * passes)
            def _():
                w_copy(m + slots).start()
        return value

    def copy1(p, slot, t):
        return remote(
            send1.at[p, slot, t], recv1.at[p, slot, t], ss1.at[p, slot, t], rs1.at[p, slot, t], (first_peer(t), s)
        )

    def copy2(p, t):
        return remote(send2.at[p, t], recv2.at[p, t], ss2.at[p, t], rs2.at[p, t], (second_peer(t), s))

    def send_out(p):
        @pl.loop(0, 2 * tiles)
        def _(m):
            slot, t = m // tiles, lax.rem(m, tiles)
            send1[p, slot, t] = mixed(p, slot, t).astype(bf16)
            copy1(p, slot, t).start()

    def pass_on(p):
        @pl.loop(0, tiles)
        def _(t):
            kept[lax.rem(p, 2), t] = mixed(p, 2, t)

        @pl.loop(0, tiles)
        def _(t):
            value = mixed(p, 3, t)
            copy1(p, 0, t).wait_recv()
            send2[p, t] = (value + recv1[p, 0, t].astype(f32)).astype(bf16)
            copy2(p, t).start()

    def collect(p):
        mine = pl.ds(pl.multiple_of(p * part, part), part)

        @pl.loop(0, tiles)
        def _(t):
            copy1(p, 1, t).wait_recv()
            copy2(p, t).wait_recv()
            value = kept[lax.rem(p, 2), t] + recv1[p, 1, t].astype(f32) + recv2[p, t].astype(f32)
            out_ref[mine, pl.ds(pl.multiple_of(t * wide, wide), wide)] = value.astype(bf16)

    id_send(z)
    kpair_stage()
    kline_stage(main, end)
    qpair_stage(0)
    qline_stage(main, 0, end)
    tables(0, s)
    id_relay()
    kline_stage(main, inner)
    kline_stage(other, True)

    @pl.when(z >= hub)
    def _():
        kv_finish(z, 0)

    @pl.loop(0, jnp.where(z == hub, hub, 0))
    def _(i):
        zz = hub - 1 - i
        tables(1, 2 * zz + c)
        kv_finish(zz, 1)

    kv_relay()

    @pl.loop(0, z + 1)
    def _(zz):
        id_pair(zz, 1 - c).wait_recv()

    @pl.loop(0, z + 1)
    def _(zz):
        kv_pair(zz, 1 - c).wait_recv()

    @pl.loop(0, pieces + 2)
    def _(p):
        more = p + 1 < pieces
        here = p < pieces

        @pl.when(more)
        def _():
            qpair_stage(p + 1)

        @pl.when((p >= 1) & (p <= pieces))
        def _():
            attend(p - 1)
            send_out(p - 1)

        qline_stage(main, p + 1, more & end)
        qline_stage(main, p, here & inner)

        @pl.when((p >= 1) & (p <= pieces))
        def _():
            pass_on(p - 1)

        qline_stage(other, p, here)

        @pl.when(p >= 2)
        def _():
            collect(p - 2)

        @pl.when(here)
        def _():
            finish(p)


    @pl.loop(0, line)
    def _(dest):
        kpair_copy(dest).wait_send()
        sent = jnp.where(jnp.maximum(dest, hub) == z, 0, 1)

        @pl.when(sent == 1)
        def _():
            kline_copy(jnp.where(jnp.maximum(dest, hub) > z, 1, 0), dest).wait_send()

        @pl.loop(0, pieces)
        def _(p):
            @pl.when(p >= pieces - 2)
            def _():
                qpair_copy(p, dest).wait_send()

            @pl.when(dest != z)
            def _():
                qline_copy(jnp.where(dest > z, 1, 0), p, dest).wait_send()

    @pl.loop(0, z + 1)
    def _(zz):
        id_pair(zz, c).wait_send()
        kv_pair(zz, c).wait_send()

        @pl.when(z < line - 1)
        def _():
            id_up(zz).wait_send()

        @pl.when((z < line - 1) & (z >= hub))
        def _():
            kv_up(zz).wait_send()

        @pl.when((zz < z) & (z <= hub))
        def _():
            kv_down(zz).wait_send()

    @pl.loop(0, pieces)
    def _(p):
        @pl.loop(0, tiles)
        def _(t):
            copy1(p, 0, t).wait_send()
            copy1(p, 1, t).wait_send()
            copy2(p, t).wait_send()


def body(seq, groups, tokens, proj_weight, proj_bias, out_weight, doc_ids):
    rows = doc_ids.shape[0]
    columns = proj_weight.shape[1]
    width = 2 * HEAD_DIM
    line = seq // 2
    part = rows // PIECES
    q_width = GQA * HEAD_DIM
    block = out_weight.shape[1] // groups
    wide = 4 * HEAD_DIM
    tiles = block // wide
    slots = 4 * tiles if line <= 4 else 2 * tiles
    inverse_freq = theta_base ** (-(jnp.arange(HEAD_DIM // 2, dtype=jnp.float32) * 2.0) / HEAD_DIM)
    freq = jnp.concatenate([inverse_freq, inverse_freq])[None, :]
    vmem = pl.BlockSpec(memory_space=pltpu.VMEM)
    dma = pltpu.SemaphoreType.DMA
    bf16, f32, i32 = jnp.bfloat16, jnp.float32, jnp.int32

    return pl.pallas_call(
        functools.partial(layer_kernel, line, rows, width, groups, tiles, wide, slots),
        out_shape=jax.ShapeDtypeStruct((rows, block), bf16),
        in_specs=[vmem] * 5 + [pl.BlockSpec(memory_space=pl.ANY)],
        out_specs=vmem,
        scratch_shapes=[
            pltpu.VMEM((line, rows, width), bf16),
            pltpu.VMEM((line, rows, width), bf16),
            pltpu.VMEM((2, line, rows, width), bf16),
            pltpu.VMEM((2, line, part, q_width), bf16),
            pltpu.VMEM((PIECES, line, part, q_width), bf16),
            pltpu.VMEM((PIECES, line + 1, part, q_width), bf16),
            pltpu.VMEM((rows, width), f32),
            pltpu.VMEM((part, q_width), f32),
            pltpu.VMEM((GQA * part, HEAD_DIM), bf16),
            pltpu.VMEM((seq, rows, width), bf16),
            pltpu.VMEM((part, q_width), bf16),
            pltpu.VMEM((rows, HEAD_DIM), i32),
            pltpu.VMEM((seq, 8, rows), i32),
            pltpu.VMEM((8, columns), f32),
            pltpu.VMEM((2, rows, HEAD_DIM), f32),
            pltpu.VMEM((2, rows, HEAD_DIM), f32),
            pltpu.VMEM((slots, q_width, wide), bf16),
            pltpu.VMEM((2, tiles, part, wide), f32),
            pltpu.VMEM((PIECES, 2, tiles, part, wide), bf16),
            pltpu.VMEM((PIECES, 2, tiles, part, wide), bf16),
            pltpu.VMEM((PIECES, tiles, part, wide), bf16),
            pltpu.VMEM((PIECES, tiles, part, wide), bf16),
        ]
        + [dma((line,)), dma((line,)), dma((line,)), dma((2, line))]
        + [dma((PIECES, line)), dma((PIECES, line)), dma((PIECES, line)), dma((PIECES, line + 1))]
        + [dma((line,))] * 9
        + [dma((slots,)), dma((PIECES, 2, tiles)), dma((PIECES, 2, tiles)), dma((PIECES, tiles)), dma((PIECES, tiles))],
        compiler_params=pltpu.CompilerParams(
            collective_id=0, has_side_effects=True, vmem_limit_bytes=67043328
        ),
        name="layer",
    )(tokens, proj_weight, proj_bias[None, :], freq, doc_ids[None, :], out_weight)


def solution(mesh):
    return jax.shard_map(
        functools.partial(body, mesh.shape["seq"], mesh.shape["grp"]),
        mesh=mesh,
        in_specs=(P(None, "seq"), P("seq", "grp"), P("grp"), P("grp", None), P("seq")),
        out_specs=P("seq", "grp"),
        check_vma=False,
    )
```

```python
import functools

import jax
import jax.numpy as jnp
import numpy as np
from jax import lax
from jax.experimental import pallas as pl
from jax.experimental.pallas import tpu as pltpu
from jax.sharding import PartitionSpec as P

HEAD_DIM = 128
GQA = 8
PARTS = (1, 1, 1, 1)
SPLITS = (2, 2, 2, 2)
MESH = pl.DeviceIdType.MESH

theta_base = 1000000.0
neg_large = -1e30
log2_e = 1.4426950408889634


def layer_kernel(
    line, rows, width, groups, tiles, wide, slots,
    bias_ref, freq_ref, ids_ref, tok_hbm, w_hbm, ow_ref,
    out_hbm,
    tok_ref, w_ref, kpair_out, kpair_in, kline_in, qpair_out, qpair_in, qline_in, ktotal, qtotal,
    queries, kv_ref, score_ref, attended, ids_col, idall_ref, first_ref, place_ref, bias, cos_ref, sin_ref,
    out_ref, weights, kept, own, send1, recv1, send2, recv2, tok_sem, in_sem, out_sem,
    kpair_ss, kpair_rs, kline_ss, kline_rs, qpair_ss, qpair_rs, qline_ss, qline_rs,
    idl_ss, idl_rs, idp_ss, idp_rs, kvu_ss, kvd_ss, kvl_rs, kvp_ss, kvp_rs,
    w_sem, ss1, rs1, ss2, rs2,
):
    g = lax.axis_index("grp")
    s = lax.axis_index("seq")
    z, c = s // 2, lax.rem(s, 2)
    n = 2 * line
    partner = s + 1 - 2 * c
    above = lax.rem(s + 2, n)
    below = lax.rem(s + n - 2, n)
    low = z < line // 2
    inner = (z > 0) & (z < line - 1)
    hub = line // 2 - 1
    pieces = len(PARTS)
    heights = [rows * k // sum(PARTS) for k in PARTS]
    starts = [sum(heights[:p]) for p in range(pieces)]
    span = line + 2
    batch = max(k for k in range(1, 7) if span % k == 0)
    steps = span // batch
    q_width = GQA * HEAD_DIM
    peer_x = g + 1 - 2 * lax.rem(g, 2)
    peer_y = lax.rem(g + 2, groups)
    passes = 4 * tiles
    resident = slots == passes
    bf16, f32 = jnp.bfloat16, jnp.float32

    def first_peer(t):
        return jnp.where(lax.rem(t, 2) == 0, peer_x, peer_y)

    def second_peer(t):
        return jnp.where(lax.rem(t, 2) == 0, peer_y, peer_x)

    def w_copy(m):
        pos, t = lax.rem(m // tiles, 4), lax.rem(m, tiles)
        block = jnp.where(
            pos == 0, groups - 1 - g, jnp.where(pos == 1, first_peer(t), jnp.where(pos == 2, g, second_peer(t)))
        )
        column = pl.multiple_of((block * tiles + t) * wide, wide)
        slot = lax.rem(m, slots)
        return pltpu.make_async_copy(ow_ref.at[:, pl.ds(column, wide)], weights.at[slot], w_sem.at[slot])

    def tok_copy(block):
        mine = pl.ds(pl.multiple_of(block * rows, rows), rows)
        return pltpu.make_async_copy(tok_hbm.at[mine, :], tok_ref.at[mine, :], tok_sem.at[block])

    kv_columns = pltpu.make_async_copy(w_hbm.at[:, q_width:], w_ref.at[:, q_width:], in_sem.at[0])
    q_columns = pltpu.make_async_copy(w_hbm.at[:, :q_width], w_ref.at[:, :q_width], in_sem.at[1])

    def far_first(i):
        return jnp.where(low, line - 1 - i, i)

    kv_columns.start()
    for core in (1 - c, c):
        @pl.loop(0, line)
        def _(i):
            tok_copy(2 * far_first(i) + core).start()

    q_columns.start()
    barrier = pltpu.get_barrier_semaphore()
    for peer in ((g, partner), (peer_x, s), (peer_y, s)):
        pl.semaphore_signal(barrier, inc=1, device_id=peer, device_id_type=MESH)

    @pl.when(z < line - 1)
    def _():
        pl.semaphore_signal(barrier, inc=1, device_id=(g, above), device_id_type=MESH)

    @pl.when(z > 0)
    def _():
        pl.semaphore_signal(barrier, inc=1, device_id=(g, below), device_id_type=MESH)

    row_ids = jnp.broadcast_to(ids_ref[...].reshape(1, rows), (HEAD_DIM, rows))
    idall_ref[s] = row_ids[:8]
    ids_col[...] = row_ids.T
    bias[...] = jnp.broadcast_to(bias_ref[...].astype(f32), bias.shape)
    pl.semaphore_wait(barrier, 3 + (z > 0).astype(jnp.int32) + (z < line - 1).astype(jnp.int32))

    def remote(src, dst, ss, rs, peer):
        return pltpu.make_async_remote_copy(src, dst, ss, rs, device_id=peer, device_id_type=MESH)


    def kpair_copy(dest):
        return remote(kpair_out.at[dest], kpair_in.at[dest], kpair_ss.at[dest], kpair_rs.at[dest], (g, partner))

    def rows_of(p):
        return pl.ds(starts[p], heights[p])

    def qpair_copy(p, dest):
        return remote(
            qpair_out.at[p % 2, dest, : heights[p]], qpair_in.at[dest, rows_of(p)],
            qpair_ss.at[p, dest], qpair_rs.at[p, dest], (g, partner),
        )

    def kline_copy(up, dest):
        return remote(
            kpair_in.at[dest], kline_in.at[up, dest], kline_ss.at[dest], kline_rs.at[up, dest],
            (g, jnp.where(up == 1, above, below)),
        )

    def strip_of(p, h):
        size = heights[p] // SPLITS[p]
        return pl.ds(starts[p] + h * size, size)

    def qline_copy(up, p, dest, h):
        return remote(
            qpair_in.at[dest, strip_of(p, h)], qline_in.at[dest + up, strip_of(p, h)],
            qline_ss.at[p, dest, h], qline_rs.at[p, dest + up, h], (g, jnp.where(up == 1, above, below)),
        )

    def kproduct(dest, core):
        row = pl.multiple_of((2 * dest + core) * rows, rows)
        return jnp.dot(tok_ref[pl.ds(row, rows), :], w_ref[:, q_width:], preferred_element_type=f32)

    def q_tokens(p, dest, core):
        return tok_ref[pl.ds(pl.multiple_of((2 * dest + core) * rows + starts[p], heights[0]), heights[p]), :]

    def kpair_stage():
        @pl.loop(0, line)
        def _(i):
            dest = far_first(i)
            tok_copy(2 * dest + 1 - c).wait()
            kpair_out[dest] = kproduct(dest, 1 - c).astype(bf16)
            kpair_copy(dest).start()

    def q_product(p, b, core):
        stacked = jnp.concatenate([q_tokens(p, 4 * b + i, core) for i in range(4)], axis=0)
        return jnp.dot(stacked, w_ref[:, :q_width], preferred_element_type=f32)

    def qpair_stage(p):
        height = heights[p]

        @pl.loop(0, line // 4)
        def _(b):
            if p >= 2:
                for i in range(4):
                    qpair_copy(p - 2, 4 * b + i).wait_send()
            value = q_product(p, b, 1 - c).astype(bf16)
            for i in range(4):
                qpair_out[p % 2, 4 * b + i, :height] = value[i * height : (i + 1) * height]
                qpair_copy(p, 4 * b + i).start()

    def qown_stage(p):
        height = heights[p]

        @pl.loop(0, line // 4)
        def _(b):
            qtotal[: 4 * height] = q_product(p, b, c)
            for i in range(4):
                dest = 4 * b + i
                qpair_copy(p, dest).wait_recv()
                qpair_in[dest, rows_of(p)] = (
                    qtotal[i * height : (i + 1) * height] + qpair_in[dest, rows_of(p)].astype(f32)
                ).astype(bf16)

    def kline_stage(up, enabled):
        count = jnp.where(up == 1, jnp.where(z < hub, line, line - 1 - z), jnp.where(z > hub, z, 0))

        @pl.loop(0, jnp.where(enabled, count, 0))
        def _(i):
            dest = jnp.where(up == 1, line - 1 - i, i)
            ktotal[...] = kproduct(dest, c)
            kpair_copy(dest).wait_recv()
            source = jnp.where(up == 1, z > 0, z < line - 1)

            @pl.when(source)
            def _():
                kline_copy(up, dest).wait_recv()
                kpair_in[dest] = (ktotal[...] + kpair_in[dest].astype(f32) + kline_in[up, dest].astype(f32)).astype(bf16)

            @pl.when(jnp.logical_not(source))
            def _():
                kpair_in[dest] = (ktotal[...] + kpair_in[dest].astype(f32)).astype(bf16)

            kline_copy(up, dest).start()

    def qline_stage(up, p, enabled):
        @pl.loop(0, jnp.where(enabled, jnp.where(up == 1, line - 1 - z, z), 0))
        def _(i):
            dest = jnp.where(up == 1, line - 1 - i, i)

            for h in range(SPLITS[p]):
                @pl.when(jnp.where(up == 1, z > 0, z < line - 1))
                def _(h=h):
                    strip = strip_of(p, h)
                    qline_copy(up, p, dest, h).wait_recv()
                    qpair_in[dest, strip] = (
                        qpair_in[dest, strip].astype(f32) + qline_in[dest + up, strip].astype(f32)
                    ).astype(bf16)

                qline_copy(up, p, dest, h).start()

    main = low.astype(jnp.int32)
    other = 1 - main
    end = jnp.logical_not(inner)


    def tables(slot, block):
        angles = (block * rows + lax.broadcasted_iota(jnp.int32, (rows, HEAD_DIM), 0)).astype(f32) * freq_ref[...]
        lane = lax.broadcasted_iota(jnp.int32, (rows, HEAD_DIM), 1)
        sine = jnp.sin(angles)
        cos_ref[slot] = jnp.cos(angles)
        sin_ref[slot] = jnp.where(lane < HEAD_DIM // 2, -sine, sine)

    def rope(x, cosine, sine):
        return x * cosine + pltpu.roll(x, HEAD_DIM // 2, 1) * sine


    def kv_up(zz):
        block = kv_ref.at[2 * zz + c]
        return remote(block, block, kvu_ss.at[zz], kvl_rs.at[zz], (g, above))

    def kv_down(zz):
        block = kv_ref.at[2 * zz + c]
        return remote(block, block, kvd_ss.at[zz], kvl_rs.at[zz], (g, below))

    def kv_pair(zz, core):
        block = kv_ref.at[2 * zz + core]
        return remote(block, block, kvp_ss.at[zz], kvp_rs.at[zz], (g, partner))

    def kv_finish(zz, slot):
        ktotal[...] = kproduct(zz, c)
        kpair_copy(zz).wait_recv()
        ktotal[...] += kpair_in[zz].astype(f32)

        @pl.when(z < line - 1)
        def _():
            kline_copy(0, zz).wait_recv()
            ktotal[...] += kline_in[0, zz].astype(f32)

        kline_copy(1, zz).wait_recv()
        value = ktotal[...] + kline_in[1, zz].astype(f32) + bias[:1, q_width:]
        kv_ref[2 * zz + c, :rows, :] = rope(value[:, :HEAD_DIM], cos_ref[slot], sin_ref[slot]).astype(bf16)
        for i in range(rows // HEAD_DIM):
            turned = value[i * HEAD_DIM : (i + 1) * HEAD_DIM, HEAD_DIM:].T
            kv_ref[2 * zz + c, rows + i * HEAD_DIM : rows + (i + 1) * HEAD_DIM, :] = turned.astype(bf16)

        @pl.when(z < line - 1)
        def _():
            kv_up(zz).start()

        @pl.when(zz < z)
        def _():
            kv_down(zz).start()

        kv_pair(zz, c).start()

    def kv_relay(begin, end):
        @pl.loop(begin, jnp.where(z > hub, jnp.minimum(z, end), begin))
        def _(i):
            zz = z - 1 - i
            kv_up(zz).wait_recv()

            @pl.when(z < line - 1)
            def _():
                kv_up(zz).start()

            kv_pair(zz, c).start()

    def kv_lower():
        @pl.loop(0, jnp.where(z < hub, z + 1, 0))
        def _(i):
            zz = z - i
            kv_down(zz).wait_recv()

            @pl.when(zz < z)
            def _():
                kv_down(zz).start()

            kv_pair(zz, c).start()


    def id_up(zz):
        block = idall_ref.at[2 * zz + c]
        return remote(block, block, idl_ss.at[zz], idl_rs.at[zz], (g, above))

    def id_pair(zz, core):
        block = idall_ref.at[2 * zz + core]
        return remote(block, block, idp_ss.at[zz], idp_rs.at[zz], (g, partner))

    def id_send(zz):
        @pl.when(z < line - 1)
        def _():
            id_up(zz).start()

        id_pair(zz, c).start()

    def id_relay():
        @pl.loop(0, z)
        def _(i):
            zz = z - 1 - i
            id_up(zz).wait_recv()
            id_send(zz)


    def finish(p):
        height = heights[p]
        cosine, sine = cos_ref[0, rows_of(p), :], sin_ref[0, rows_of(p), :]

        @pl.when(z < line - 1)
        def _():
            for h in range(SPLITS[p]):
                qline_copy(0, p, z, h).wait_recv()

        @pl.when(z > 0)
        def _():
            for h in range(SPLITS[p]):
                qline_copy(1, p, z, h).wait_recv()

        def turn(sources):
            for head in range(GQA):
                lanes = slice(head * HEAD_DIM, (head + 1) * HEAD_DIM)
                value = qpair_in[z, rows_of(p), lanes].astype(f32) + bias[:1, lanes]
                for source in sources:
                    value = value + qline_in[source, rows_of(p), lanes].astype(f32)
                queries[head * height : (head + 1) * height, :] = rope(value, cosine, sine).astype(bf16)

        @pl.when(inner)
        def _():
            turn((z, z + 1))

        @pl.when(z == 0)
        def _():
            turn((z,))

        @pl.when(z == line - 1)
        def _():
            turn((z + 1,))


    def places():
        @pl.loop(0, z + 1)
        def _(zz):
            id_pair(zz, 1 - c).wait_recv()

        def step(j, count):
            return count + jnp.where(idall_ref[j, :1, :] < ids_col[:, :1], 1.0, 0.0)

        count = lax.fori_loop(0, s + 1, step, jnp.zeros((rows, rows), f32))
        first = jnp.broadcast_to(jnp.sum(count, axis=1, keepdims=True), (rows, HEAD_DIM))
        first = jnp.concatenate(
            [first[i * HEAD_DIM : (i + 1) * HEAD_DIM].T for i in range(rows // HEAD_DIM)], axis=1
        )[:8].astype(jnp.int32)
        place = s * rows + lax.broadcasted_iota(jnp.int32, (8, rows), 1)
        for p in range(pieces):
            lanes = slice(starts[p], starts[p] + heights[p])
            first_ref[p] = jnp.concatenate([first[:, lanes]] * (rows // heights[p]), axis=1)
            place_ref[p] = jnp.concatenate([place[:, lanes]] * (rows // heights[p]), axis=1)

    def attend(p):
        height = heights[p]
        heads = rows // height
        stacks = GQA // heads
        lanes = rows
        key = lax.broadcasted_iota(jnp.int32, (rows, lanes), 0)
        ones = jnp.ones((16, rows), bf16)
        scale = HEAD_DIM ** (-0.5) * log2_e
        start = s - (line + 1)

        def step(k, state):
            highest = [state[i][0] for i in range(stacks)]
            for n in range(batch):
                j = start + k * batch + n
                block = jnp.maximum(j, 0)
                keys = kv_ref[block, :rows, :]
                allowed = (key >= first_ref[p, :1, :] - j * rows) & (key <= place_ref[p, :1, :] - j * rows)
                for i in range(stacks):
                    scores = lax.dot_general(
                        keys, queries[i * lanes : (i + 1) * lanes, :], (((1,), (1,)), ((), ())),
                        preferred_element_type=f32,
                    )
                    scores = jnp.where(allowed, scores * scale, neg_large)
                    score_ref[i, n * rows : (n + 1) * rows, :] = scores
                    highest[i] = jnp.maximum(highest[i], jnp.max(scores.reshape(rows // 8, 8, lanes), axis=0))
            new = []
            for i in range(stacks):
                row_max, weighted = state[i]
                new_max = jnp.broadcast_to(jnp.max(highest[i], axis=0, keepdims=True), (8, lanes))
                update = jnp.zeros((HEAD_DIM + 16, lanes), f32)
                for n in range(batch):
                    block = jnp.maximum(start + k * batch + n, 0)
                    turned = [
                        kv_ref[block, rows + m * HEAD_DIM : rows + (m + 1) * HEAD_DIM, :] for m in range(rows // HEAD_DIM)
                    ]
                    values = jnp.concatenate([jnp.concatenate(turned, axis=1), ones], axis=0)
                    exps = jnp.exp2(score_ref[i, n * rows : (n + 1) * rows, :] - new_max[:1])
                    update = update + jnp.dot(values, exps.astype(bf16), preferred_element_type=f32)
                if steps > 1:
                    update = weighted * jnp.exp2(row_max[:1] - new_max[:1]) + update
                new.append((new_max, update))
            return tuple(new)

        initial = (jnp.full((8, lanes), neg_large, f32), jnp.zeros((HEAD_DIM + 16, lanes), f32))
        if steps > 1:
            state = lax.fori_loop(0, steps, step, (initial,) * stacks)
        else:
            state = step(0, (initial,) * stacks)
        for i in range(stacks):
            weighted = state[i][1]
            value = weighted[:HEAD_DIM] / weighted[HEAD_DIM : HEAD_DIM + 1]
            for k in range(lanes // HEAD_DIM):
                block = value[:, k * HEAD_DIM : (k + 1) * HEAD_DIM].T.astype(bf16)
                for h in range(HEAD_DIM // height):
                    head = i * heads + k * (HEAD_DIM // height) + h
                    attended[:height, head * HEAD_DIM : (head + 1) * HEAD_DIM] = block[h * height : (h + 1) * height]


    def mixed(p, pos, t):
        m = p * passes + pos * tiles + t
        slot = lax.rem(m, slots)
        if not resident:
            w_copy(m).wait()
        value = jnp.dot(attended[: heights[p]], weights[slot], preferred_element_type=f32)
        if not resident:
            @pl.when(m + slots < pieces * passes)
            def _():
                w_copy(m + slots).start()
        return value

    def mixed_tiles(p, pos, begin, count):
        if not resident:
            return [mixed(p, pos, begin + i) for i in range(count)]
        joined = jnp.concatenate([weights[pos * tiles + begin + i] for i in range(count)], axis=1)
        value = jnp.dot(attended[: heights[p]], joined, preferred_element_type=f32)
        return [value[:, i * wide : (i + 1) * wide] for i in range(count)]

    def copy1(p, slot, t):
        return remote(
            send1.at[slot, t, rows_of(p)], recv1.at[slot, t, rows_of(p)], ss1.at[p, slot, t], rs1.at[p, slot, t], (first_peer(t), s)
        )

    def copy2(p, t):
        return remote(send2.at[t, rows_of(p)], recv2.at[t, rows_of(p)], ss2.at[p, t], rs2.at[p, t], (second_peer(t), s))

    def send_out(p):
        if resident and p == 0:
            @pl.loop(0, slots)
            def _(m):
                w_copy(m).wait()

        @pl.loop(0, 2)
        def _(slot):
            for begin in range(0, tiles, 2):
                for i, value in enumerate(mixed_tiles(p, slot, begin, 2)):
                    send1[slot, begin + i, rows_of(p)] = value.astype(bf16)
                    copy1(p, slot, begin + i).start()

    def pass_on(p):
        for begin in range(0, tiles, 4):
            for i, value in enumerate(mixed_tiles(p, 2, begin, 4)):
                kept[begin + i, rows_of(p)] = value
        for begin in range(0, tiles, 4):
            for i, value in enumerate(mixed_tiles(p, 3, begin, 4)):
                own[begin + i, : heights[p]] = value

        @pl.loop(0, tiles)
        def _(t):
            copy1(p, 0, t).wait_recv()
            send2[t, rows_of(p)] = (own[t, : heights[p]] + recv1[0, t, rows_of(p)].astype(f32)).astype(bf16)
            copy2(p, t).start()

    def out_copy(p):
        return pltpu.make_async_copy(out_ref.at[rows_of(p), :], out_hbm.at[rows_of(p), :], out_sem.at[p])

    def collect(p):
        @pl.loop(0, tiles)
        def _(t):
            copy1(p, 1, t).wait_recv()
            copy2(p, t).wait_recv()
            value = kept[t, rows_of(p)] + recv1[1, t, rows_of(p)].astype(f32) + recv2[t, rows_of(p)].astype(f32)
            out_ref[rows_of(p), pl.ds(pl.multiple_of(t * wide, wide), wide)] = value.astype(bf16)

        out_copy(p).start()

    def settle():
        @pl.loop(0, line)
        def _(dest):
            kpair_copy(dest).wait_send()
            sent = jnp.where(jnp.maximum(dest, hub) == z, 0, 1)

            @pl.when(sent == 1)
            def _():
                kline_copy(jnp.where(jnp.maximum(dest, hub) > z, 1, 0), dest).wait_send()

            for p in range(pieces):
                if p >= pieces - 2:
                    qpair_copy(p, dest).wait_send()

                @pl.when(dest != z)
                def _(p=p):
                    for h in range(SPLITS[p]):
                        qline_copy(jnp.where(dest > z, 1, 0), p, dest, h).wait_send()

        @pl.loop(0, z + 1)
        def _(zz):
            id_pair(zz, c).wait_send()
            kv_pair(zz, c).wait_send()

            @pl.when(z < line - 1)
            def _():
                id_up(zz).wait_send()

            @pl.when((z < line - 1) & (z >= hub))
            def _():
                kv_up(zz).wait_send()

            @pl.when((zz < z) & (z <= hub))
            def _():
                kv_down(zz).wait_send()

    def query_stage(p):
        qown_stage(p)
        qline_stage(main, p, end)

    id_send(z)
    kv_columns.wait()
    kpair_stage()

    @pl.loop(0, line)
    def _(dest):
        tok_copy(2 * dest + c).wait()

    kline_stage(main, end)
    q_columns.wait()

    @pl.loop(0, slots)
    def _(m):
        w_copy(m).start()

    qpair_stage(0)
    qpair_stage(1)
    query_stage(0)
    id_relay()
    kline_stage(main, inner)
    kline_stage(other, True)

    for p in range(1, pieces):
        if p + 1 < pieces:
            qpair_stage(p + 1)
        query_stage(p)

    @pl.loop(0, jnp.where(z == hub, 2, 1))
    def _(i):
        tables(i, jnp.where(i == 0, s, s - 2))

    places()

    @pl.when(z >= hub)
    def _():
        kv_finish(z, 0)

    @pl.loop(0, jnp.where(z == hub, hub, 0))
    def _(i):
        zz = hub - 1 - i

        @pl.when(i > 0)
        def _():
            tables(1, 2 * zz + c)

        kv_finish(zz, 1)

    kv_relay(0, 1)
    qline_stage(main, 0, inner)
    kv_relay(1, line)
    kv_lower()

    @pl.loop(0, z + 1)
    def _(zz):
        kv_pair(zz, 1 - c).wait_recv()

    for p in range(pieces + 2):
        here = p < pieces
        relay = here and p > 0
        if relay:
            qline_stage(main, p, inner & jnp.logical_not(low))
        if 1 <= p <= pieces:
            attend(p - 1)
            send_out(p - 1)
        if relay:
            qline_stage(main, p, inner & low)
        if here:
            qline_stage(other, p, True)
        if p == pieces:
            settle()
        if 1 <= p <= pieces:
            pass_on(p - 1)
        if p >= 2:
            collect(p - 2)
        if here:
            finish(p)


    for p in range(pieces):
        @pl.loop(0, tiles)
        def _(t):
            copy1(p, 0, t).wait_send()
            copy1(p, 1, t).wait_send()
            copy2(p, t).wait_send()

        out_copy(p).wait()


def body(seq, groups, tokens, proj_weight, proj_bias, out_weight, doc_ids):
    rows = doc_ids.shape[0]
    columns = proj_weight.shape[1]
    width = 2 * HEAD_DIM
    line = seq // 2
    part = rows * max(PARTS) // sum(PARTS)
    pieces = len(PARTS)
    q_width = GQA * HEAD_DIM
    block = out_weight.shape[1] // groups
    wide = 4 * HEAD_DIM
    tiles = block // wide
    slots = 4 * tiles if line <= 4 else 2 * tiles
    inverse_freq = (theta_base ** (-np.arange(HEAD_DIM // 2) * 2.0 / HEAD_DIM)).astype(np.float32)
    freq = jnp.asarray(np.concatenate([inverse_freq, inverse_freq])[None, :])
    vmem = pl.BlockSpec(memory_space=pltpu.VMEM)
    dma = pltpu.SemaphoreType.DMA
    bf16, f32, i32 = jnp.bfloat16, jnp.float32, jnp.int32

    return pl.pallas_call(
        functools.partial(layer_kernel, line, rows, width, groups, tiles, wide, slots),
        out_shape=jax.ShapeDtypeStruct((rows, block), bf16),
        in_specs=[vmem] * 3 + [pl.BlockSpec(memory_space=pl.ANY)] * 3,
        out_specs=pl.BlockSpec(memory_space=pl.ANY),
        scratch_shapes=[
            pltpu.VMEM(tokens.shape, bf16),
            pltpu.VMEM(proj_weight.shape, bf16),
            pltpu.VMEM((line, rows, width), bf16),
            pltpu.VMEM((line, rows, width), bf16),
            pltpu.VMEM((2, line, rows, width), bf16),
            pltpu.VMEM((2, line, part, q_width), bf16),
            pltpu.VMEM((line, rows, q_width), bf16),
            pltpu.VMEM((line + 1, rows, q_width), bf16),
            pltpu.VMEM((rows, width), f32),
            pltpu.VMEM((4 * part, q_width), f32),
            pltpu.VMEM((GQA * part, HEAD_DIM), bf16),
            pltpu.VMEM((seq, 2 * rows, HEAD_DIM), bf16),
            pltpu.VMEM((GQA * part // rows, 6 * rows, rows), f32),
            pltpu.VMEM((part, q_width), bf16),
            pltpu.VMEM((rows, HEAD_DIM), i32),
            pltpu.VMEM((seq, 8, rows), i32),
            pltpu.VMEM((pieces, 8, rows), i32),
            pltpu.VMEM((pieces, 8, rows), i32),
            pltpu.VMEM((8, columns), f32),
            pltpu.VMEM((2, rows, HEAD_DIM), f32),
            pltpu.VMEM((2, rows, HEAD_DIM), f32),
            pltpu.VMEM((rows, block), bf16),
            pltpu.VMEM((slots, q_width, wide), bf16),
            pltpu.VMEM((tiles, rows, wide), f32),
            pltpu.VMEM((tiles, part, wide), f32),
            pltpu.VMEM((2, tiles, rows, wide), bf16),
            pltpu.VMEM((2, tiles, rows, wide), bf16),
            pltpu.VMEM((tiles, rows, wide), bf16),
            pltpu.VMEM((tiles, rows, wide), bf16),
        ]
        + [dma((seq,)), dma((2,)), dma((pieces,))]
        + [dma((line,)), dma((line,)), dma((line,)), dma((2, line))]
        + [dma((pieces, line)), dma((pieces, line)), dma((pieces, line, 2)), dma((pieces, line + 1, 2))]
        + [dma((line,))] * 9
        + [dma((slots,)), dma((pieces, 2, tiles)), dma((pieces, 2, tiles)), dma((pieces, tiles)), dma((pieces, tiles))],
        compiler_params=pltpu.CompilerParams(
            collective_id=0, has_side_effects=True, vmem_limit_bytes=67043328
        ),
        name="layer",
    )(proj_bias, freq, doc_ids[None, :], tokens, proj_weight, out_weight)


def solution(mesh):
    return jax.shard_map(
        functools.partial(body, mesh.shape["seq"], mesh.shape["grp"]),
        mesh=mesh,
        in_specs=(P(None, "seq"), P("seq", "grp"), P("grp"), P("grp", None), P("seq")),
        out_specs=P("seq", "grp"),
        check_vma=False,
    )
```
